512 devices in a mesh: snap: 2 (over y), row: 128 (over z, x), col: 2 (over core).
Axes of the slice: x: 8, y: 2, z: 16, core: 2. Of those that a mesh axis runs over, the one named last changes fastest.
The devices are a block of a 8x8x16 slice.
Arguments:
- density: bfloat16 [131072, 1024], P(('snap', 'row'), 'col'), parts along dimension 0, may hold values from -0.5 to 2
- pattern: int32 [4096, 32], P(('snap', 'row'), 'col'), parts along dimension 0, may hold values 0 or 1
- filter_mask: int32 [4096, 32], P(('snap', 'row')), parts along dimension 0, may hold values 0 or 1
Outputs:
- purified: bfloat16 [131072, 1024], P(('snap', 'row'), 'col'), parts along dimension 0
- traces: float32 [4], P('snap'), parts along dimension 0
The draws below stay inside these ranges and needn't reach their ends.
There are 2 independent parts, one for each index of `snap`. The reference program is written for one: setup_inputs(seed, part) draws one part's arguments, and reference() takes and returns one part's arrays. A program takes and returns all parts, laid end to end along the dimension named above; each array names one. Nothing has to cross between parts.
All inputs are finite; a program needn't handle non-finite values. No bound on the sum of `pattern` or of `filter_mask` on one device may be relied on, other than what follows from the above.
Results may differ from the reference program's by a relative error of at most 0.006.
Values may be sent and summed in bfloat16 or wider, within the bound.
No kernel may reach another device: no remote copies, remote signals or barrier semaphores. Data moves between devices by JAX's collectives and lax.ppermute only.
A program may use at most 64 MiB of HBM per device.

```python
import jax
import jax.numpy as jnp
from jax import lax

BLK = 32
S = 32
H = 16
NB = 2048
ORDER = 65536


def draw_density(key, part):
    keys = jax.random.split(jax.random.fold_in(key, 11), 2)
    width = S * BLK
    sigma = 0.9 / width ** 0.5
    row_index = jnp.arange(ORDER, dtype=jnp.int32)
    offdiag = jnp.clip(jax.random.normal(keys[0], (ORDER, width), jnp.float32), -4.5, 4.5) * sigma
    rising = 0.3 + 0.6 * row_index.astype(jnp.float32) / ORDER
    occupied = jax.random.uniform(keys[1], (ORDER,), jnp.float32, 0.5, 1.5) * rising
    column_index = jnp.arange(width, dtype=jnp.int32)
    on_diagonal = column_index[None, :] == (H * BLK + row_index % BLK)[:, None]
    values = offdiag + jnp.where(on_diagonal, occupied[:, None], 0.0)
    return values.astype(jnp.bfloat16)


def place_ends(drawn, stream_key, smallest, top_value):
    longest = drawn.shape.index(max(drawn.shape))
    spots = []
    for shift in (0, 1):
        where = [jax.random.randint(jax.random.fold_in(stream_key, axis), (), 0, length) for axis, length in enumerate(drawn.shape)]
        where[longest] = (where[longest] + shift) % drawn.shape[longest]
        spots.append(tuple(where))
    return drawn.at[spots[0]].set(smallest).at[spots[1]].set(top_value)


def setup_inputs(seed: int = 0, part: int = 0) -> dict:
    streams_of = jax.random.split(jax.random.key(seed), 4)
    part_splits = jax.random.split(jax.random.fold_in(streams_of[3], part), 4)
    return {
        "density": draw_density(jax.random.fold_in(jax.random.fold_in(streams_of[3], part), 71), part),
        "pattern": place_ends((jax.random.randint(part_splits[1], (NB, S), 0, 4) < 3).astype(jnp.int32), jax.random.fold_in(part_splits[1], 1), 0, 1),
        "filter_mask": place_ends((jax.random.randint(part_splits[2], (NB, S), 0, 8) < 7).astype(jnp.int32), jax.random.fold_in(part_splits[2], 1), 0, 1),
    }


def valid_slots(row_total, slot_count, half_band):
    row_index = jnp.arange(row_total, dtype=jnp.int32)
    slot_index = jnp.arange(slot_count, dtype=jnp.int32)
    column_index = row_index[:, None] + slot_index[None, :] - half_band
    return ((column_index >= 0) & (column_index < row_total)).astype(jnp.int32)


def expand_mask(values, keep_mask):
    block_rows = keep_mask.shape[0]
    slot_count = keep_mask.shape[1]
    blocks = values.reshape(block_rows, BLK, slot_count, BLK)
    blocks = blocks * keep_mask.astype(values.dtype)[:, None, :, None]
    return blocks.reshape(block_rows * BLK, slot_count * BLK)


def shift_slots(segment, moved):
    height = segment.shape[0]
    if moved > 0:
        return jnp.concatenate([jnp.zeros((height, moved * BLK), segment.dtype), segment[:, : segment.shape[1] - moved * BLK]], 1)
    if moved < 0:
        return jnp.concatenate([segment[:, -moved * BLK:], jnp.zeros((height, -moved * BLK), segment.dtype)], 1)
    return segment


def band_product(left, right):
    group_rows = 8 if NB % 8 == 0 else 2
    extended = jnp.pad(right, ((H * BLK, H * BLK), (0, 0)))

    def one_group(group):
        first = group * group_rows
        stacked = []
        for offset in range(S):
            segment = lax.dynamic_slice_in_dim(extended, (first + offset) * BLK, group_rows * BLK, 0)
            segment = shift_slots(segment, offset - H)
            stacked.append(segment.reshape(group_rows, BLK, S * BLK))
        gathered = jnp.stack(stacked, 1).reshape(group_rows, S * BLK, S * BLK).astype(jnp.float32)
        left_rows = lax.dynamic_slice_in_dim(left, first * BLK, group_rows * BLK, 0)
        left_rows = left_rows.reshape(group_rows, BLK, S * BLK).astype(jnp.float32)
        result = jnp.einsum("gak,gkn->gan", left_rows, gathered)
        return result.reshape(group_rows * BLK, S * BLK)

    result = lax.map(one_group, jnp.arange(NB // group_rows, dtype=jnp.int32))
    return result.reshape(NB * BLK, S * BLK)


def diagonal_sum(values):
    blocks = values.reshape(NB, BLK, S, BLK)[:, :, H, :]
    return jnp.sum(jnp.diagonal(blocks, axis1=1, axis2=2).astype(jnp.float32))


def reference(density, pattern, filter_mask):
    valid = valid_slots(NB, S, H)
    kept = expand_mask(density, pattern * valid)
    square = band_product(kept, kept)
    keep_filter = filter_mask * valid
    squared = expand_mask(square, keep_filter).astype(jnp.bfloat16)
    cube = band_product(squared, kept)
    purified = (3.0 * squared.astype(jnp.float32) - 2.0 * expand_mask(cube, keep_filter)).astype(jnp.bfloat16)
    traces = jnp.stack([diagonal_sum(kept), diagonal_sum(squared)]) / ORDER
    return purified, traces
```

```python
import functools

import jax
import jax.numpy as jnp
from jax import lax
from jax.experimental import pallas as pl
from jax.experimental.pallas import tpu as pltpu
from jax.sharding import PartitionSpec as P

BLK = 32
LANES = 128
TILE = 256
SNAP_ROW = ("snap", "row")


def spread(mask, width):
    slots = mask.shape[1]
    slot = lax.broadcasted_iota(jnp.int32, (slots, width), 0)
    lane = lax.broadcasted_iota(jnp.int32, (slots, width), 1)
    chosen = (lane // BLK == slot).astype(jnp.bfloat16)
    return jnp.dot(
        mask.astype(jnp.bfloat16), chosen, preferred_element_type=jnp.float32
    )


def placed(rows, start, width):
    height, length = rows.shape
    if start < 0:
        rows = rows[:, -start:]
        length += start
        start = 0
    if start + length > width:
        length = width - start
        rows = rows[:, :length]
    parts = []
    if start:
        parts.append(jnp.zeros((height, start), rows.dtype))
    parts.append(rows)
    if start + length < width:
        parts.append(jnp.zeros((height, width - start - length), rows.dtype))
    return jnp.concatenate(parts, 1) if len(parts) > 1 else rows


def eye_sum(ref, lane_start):
    row = lax.broadcasted_iota(jnp.int32, (LANES, LANES), 0)
    lane = lax.broadcasted_iota(jnp.int32, (LANES, LANES), 1)
    total = jnp.zeros((1, LANES), jnp.float32)
    for k in range(ref.shape[0] // LANES):
        part = ref[pl.ds(k * LANES, LANES), pl.ds(lane_start + k * LANES, LANES)]
        part = jnp.where(row == lane, part.astype(jnp.float32), 0.0)
        total += jnp.sum(part, axis=0, keepdims=True)
    return total


def purify_kernel(
    col_ref, filter_ref, own_a, own_b, up_a, up_b, low_a, low_b,
    out_ref, trace_ref, band, full, sq, fmask, cube, sems,
):
    height, half = own_a.shape
    block_rows = height // BLK
    slots = 2 * half // BLK
    col = col_ref[0]
    mine = pl.multiple_of(col * half, half)
    other = pl.multiple_of((1 - col) * half, half)
    copies = []
    for k, (src, row, lane) in enumerate((
        (own_a, 1, mine), (own_b, 1, other), (up_a, 0, mine),
        (up_b, 0, other), (low_a, 2, mine), (low_b, 2, other),
    )):
        copy = pltpu.make_async_copy(
            src, band.at[pl.ds(row * height, height), pl.ds(lane, half)], sems.at[k]
        )
        copy.start()
        copies.append(copy)
    width = full.shape[1]
    wide = spread(filter_ref[...], slots * BLK)
    for i in range(block_rows):
        fmask[pl.ds(i, 1), :] = placed(wide[i : i + 1], i * BLK, width)

    def skew(row):
        for r in range(row * block_rows, (row + 1) * block_rows):
            rows = band[pl.ds(r * BLK, BLK), :]
            full[pl.ds(r * BLK, BLK), :] = placed(rows, (r - block_rows) * BLK, width)

    copies[0].wait()
    copies[1].wait()
    skew(1)
    trace_ref[...] = jnp.zeros_like(trace_ref)
    trace_ref[pl.ds(0, 1), :] = eye_sum(full.at[pl.ds(height, height), :], height)
    copies[2].wait()
    copies[3].wait()
    skew(0)
    copies[4].wait()
    copies[5].wait()
    skew(2)
    tiles = height // TILE
    span = (block_rows * 2 + TILE // BLK - 1) * BLK
    span = -(-span // TILE)
    reach = height // TILE
    per_tile = TILE // BLK
    sq[...] = jnp.zeros_like(sq)
    for m in range(tiles):
        for b in range(m, m + span):
            first = max(b - reach, m)
            last = min(b + reach, m + span - 1)
            k0, klen = first * TILE, (last - first + 1) * TILE
            prod = jnp.dot(
                full[pl.ds(height + m * TILE, TILE), pl.ds(k0, klen)],
                full[pl.ds(k0, klen), pl.ds(b * TILE, TILE)],
                preferred_element_type=jnp.float32,
            )
            for i in range(per_tile):
                row = m * per_tile + i
                keep = fmask[pl.ds(row, 1), pl.ds(b * TILE, TILE)]
                sq[pl.ds(row * BLK, BLK), pl.ds(b * TILE, TILE)] = (
                    prod[i * BLK : (i + 1) * BLK] * keep
                ).astype(jnp.bfloat16)
    trace_ref[pl.ds(1, 1), :] = eye_sum(sq, height)
    out_span = half // TILE + 1
    for m in range(tiles):
        lanes = pl.multiple_of(m * TILE + col * half, TILE)
        cube[...] = jnp.dot(
            sq[pl.ds(m * TILE, TILE), pl.ds(m * TILE, span * TILE)],
            full[pl.ds(m * TILE, span * TILE), pl.ds(lanes, out_span * TILE)],
            preferred_element_type=jnp.float32,
        )
        for i in range(per_tile):
            row = m * per_tile + i
            base = i * BLK // LANES * LANES
            shift = i * BLK - base
            size = half + (LANES if shift else 0)
            at = pl.ds(pl.multiple_of(m * TILE + base + col * half, LANES), size)
            kept = sq[pl.ds(row * BLK, BLK), at].astype(jnp.float32)
            keep = fmask[pl.ds(row, 1), at]
            part = cube[pl.ds(i * BLK, BLK), pl.ds(base, size)]
            result = (3.0 * kept - 2.0 * (part * keep)).astype(jnp.bfloat16)
            out_ref[pl.ds(row * BLK, BLK), :] = result[:, shift : shift + half]


def purify(col, keep_filter, *pieces):
    height, half = pieces[0].shape
    width = 3 * height
    block_rows = height // BLK
    anywhere = pl.BlockSpec(memory_space=pl.ANY)
    vmem = pl.BlockSpec(memory_space=pltpu.VMEM)
    return pl.pallas_call(
        purify_kernel,
        out_shape=(
            jax.ShapeDtypeStruct((height, half), jnp.bfloat16),
            jax.ShapeDtypeStruct((8, LANES), jnp.float32),
        ),
        in_specs=[pl.BlockSpec(memory_space=pltpu.SMEM), vmem] + [anywhere] * 6,
        out_specs=(vmem, vmem),
        scratch_shapes=[
            pltpu.VMEM((width, 2 * half), jnp.bfloat16),
            pltpu.VMEM((width, width), jnp.bfloat16),
            pltpu.VMEM((height, width), jnp.bfloat16),
            pltpu.VMEM((block_rows, width), jnp.float32),
            pltpu.VMEM((TILE, half + TILE), jnp.float32),
            pltpu.SemaphoreType.DMA((6,)),
        ],
        compiler_params=pltpu.CompilerParams(vmem_limit_bytes=48 * 1024 * 1024),
        cost_estimate=pl.CostEstimate(flops=3 * 10**9, bytes_accessed=4 * 10**6, transcendentals=0),
        name="purify",
    )(col, keep_filter, *pieces)


def valid_slots(first_row, row_count, first_slot, slot_count, half_band, block_total):
    row_index = first_row + jnp.arange(row_count, dtype=jnp.int32)
    slot_index = first_slot + jnp.arange(slot_count, dtype=jnp.int32)
    column_index = row_index[:, None] + slot_index[None, :] - half_band
    return ((column_index >= 0) & (column_index < block_total)).astype(jnp.int32)


def expand_mask(values, keep_mask):
    block_rows, slot_count = keep_mask.shape
    blocks = values.reshape(block_rows, BLK, slot_count, BLK)
    blocks = blocks * keep_mask.astype(values.dtype)[:, None, :, None]
    return blocks.reshape(block_rows * BLK, slot_count * BLK)


def swapped(value):
    return lax.ppermute(value, "col", [(0, 1), (1, 0)])


def per_device(density, pattern, filter_mask):
    half_slots = density.shape[1] // BLK
    slot_count = 2 * half_slots
    block_rows = density.shape[0] // BLK
    col = lax.axis_index("col")
    row = lax.axis_index("row")
    size = lax.axis_size("row")
    block_total = block_rows * size
    valid = valid_slots(row * block_rows, block_rows, 0, slot_count, half_slots, block_total)
    own_valid = lax.dynamic_slice_in_dim(valid, col * half_slots, half_slots, 1)
    kept = expand_mask(density, pattern * own_valid)
    up = lax.ppermute(kept, "row", [(i, (i + 1) % size) for i in range(size)])
    low = lax.ppermute(kept, "row", [((i + 1) % size, i) for i in range(size)])
    own_b = swapped(kept)
    up_b, low_b = swapped(up), swapped(low)
    purified, sums = purify(
        col.reshape(1).astype(jnp.int32), filter_mask * valid, kept, own_b, up, up_b, low, low_b
    )
    sums = jnp.sum(sums[:2], axis=1)
    spread_sums = jnp.zeros((1, LANES), jnp.float32).at[0, :2].set(sums)
    copies = jnp.broadcast_to(spread_sums[None], (size, 1, LANES))
    copies = lax.all_to_all(copies, "row", split_axis=0, concat_axis=0, tiled=True)
    traces = jnp.sum(copies, axis=(0, 1))[:2] / (block_total * BLK)
    return purified, traces


def solution(mesh):
    placed_as = (P(SNAP_ROW, "col"), P(SNAP_ROW, "col"), P(SNAP_ROW, None))
    return jax.shard_map(
        per_device,
        mesh=mesh,
        in_specs=placed_as,
        out_specs=(P(SNAP_ROW, "col"), P("snap")),
        check_vma=False,
    )
```

```python
import jax
import jax.numpy as jnp
from jax import lax
from jax.experimental import pallas as pl
from jax.experimental.pallas import tpu as pltpu
from jax.sharding import PartitionSpec as P


BLK = 32
LANES = 128
TILE = 256
SNAP_ROW = ("snap", "row")


def spread(mask, width):
    slots = mask.shape[1]
    slot = lax.broadcasted_iota(jnp.int32, (slots, width), 0)
    lane = lax.broadcasted_iota(jnp.int32, (slots, width), 1)
    chosen = (lane // BLK == slot).astype(jnp.bfloat16)
    return jnp.dot(
        mask.astype(jnp.bfloat16), chosen, preferred_element_type=jnp.float32
    )


def placed(rows, start, width):
    height, length = rows.shape
    if start < 0:
        rows = rows[:, -start:]
        length += start
        start = 0
    if start + length > width:
        length = width - start
        rows = rows[:, :length]
    parts = []
    if start:
        parts.append(jnp.zeros((height, start), rows.dtype))
    parts.append(rows)
    if start + length < width:
        parts.append(jnp.zeros((height, width - start - length), rows.dtype))
    return jnp.concatenate(parts, 1) if len(parts) > 1 else rows


def eye_sum(ref, lane_start):
    row = lax.broadcasted_iota(jnp.int32, (LANES, LANES), 0)
    lane = lax.broadcasted_iota(jnp.int32, (LANES, LANES), 1)
    total = jnp.zeros((1, LANES), jnp.float32)
    for k in range(ref.shape[0] // LANES):
        part = ref[pl.ds(k * LANES, LANES), pl.ds(lane_start + k * LANES, LANES)]
        part = jnp.where(row == lane, part.astype(jnp.float32), 0.0)
        total += jnp.sum(part, axis=0, keepdims=True)
    return total


def own_valid(scalars, block_rows, first_slot, slots, half_band):
    row = lax.broadcasted_iota(jnp.int32, (block_rows, slots), 0)
    slot = lax.broadcasted_iota(jnp.int32, (block_rows, slots), 1)
    column = scalars[1] + row + first_slot + slot - half_band
    return (column >= 0) & (column < scalars[2])


def keep_kernel(scalars, density, pattern, keep_filter, kept):
    height, half = density.shape
    block_rows, slots = pattern.shape
    valid = own_valid(scalars, block_rows, scalars[0] * slots, slots, slots)
    mask = spread(jnp.where(valid, pattern[...], 0), half).astype(jnp.bfloat16)
    for i in range(block_rows):
        rows = pl.ds(i * BLK, BLK)
        kept[rows, :] = density[rows, :] * mask[i : i + 1]
    slot = lax.broadcasted_iota(jnp.int32, keep_filter.shape, 1)
    on_diagonal = jnp.where(slot == slots, keep_filter[...], 0).astype(jnp.float32)
    on_diagonal = jnp.sum(on_diagonal, axis=1, keepdims=True)
    kept[pl.ds(height, block_rows), :] = jnp.broadcast_to(
        on_diagonal, (block_rows, half)
    ).astype(jnp.bfloat16)


def keep(scalars, density, pattern, keep_filter):
    height, half = density.shape
    vmem = pl.BlockSpec(memory_space=pltpu.VMEM)
    return pl.pallas_call(
        keep_kernel,
        out_shape=jax.ShapeDtypeStruct((height + pattern.shape[0], half), jnp.bfloat16),
        in_specs=[pl.BlockSpec(memory_space=pltpu.SMEM), vmem, vmem, vmem],
        out_specs=vmem,
        compiler_params=pltpu.CompilerParams(vmem_limit_bytes=16 * 1024 * 1024),
        cost_estimate=pl.CostEstimate(flops=10**9, bytes_accessed=10**6, transcendentals=0),
        name="keep",
    )(scalars, density, pattern, keep_filter)


def joined(left, right):
    parts = [part for part in (left, right) if part.shape[1]]
    return jnp.concatenate(parts, 1) if len(parts) > 1 else parts[0]


def weighted_diagonal(a, b, weight):
    total = jnp.zeros((1, TILE), jnp.float32)
    row = lax.broadcasted_iota(jnp.int32, (TILE, TILE), 0)
    lane = lax.broadcasted_iota(jnp.int32, (TILE, TILE), 1)
    for m in range(a.shape[0] // TILE):
        at = pl.ds(m * TILE, TILE)
        prod = jnp.dot(a[at, :], b[:, at], preferred_element_type=jnp.float32)
        diagonal = jnp.sum(jnp.where(row == lane, prod, 0.0), axis=0, keepdims=True)
        total += diagonal * weight[:, m * TILE : (m + 1) * TILE]
    return jnp.sum(total)


def trace_kernel(
    scalars, own_a, own_b, near, out_ref, left, right, upper, lower, square, x_ref, y_ref, sems
):
    half = own_a.shape[1]
    height = square.shape[0]
    block_rows = height // BLK
    col = scalars[0]

    def fetch(sources):
        copies = [
            pltpu.make_async_copy(src, dst, sems.at[k])
            for k, (src, dst) in enumerate(zip(sources, (left, right, upper, lower)))
        ]
        for copy in copies:
            copy.start()
        for copy in copies:
            copy.wait()

    @pl.when(col == 0)
    def _():
        fetch((own_a, own_b, near, own_a))

    @pl.when(col != 0)
    def _():
        fetch((own_b, own_a, own_a, near))

    for i in range(block_rows):
        rows = pl.ds(i * BLK, BLK)
        cut = half - i * BLK
        square[rows, :] = joined(left[rows, :][:, cut:], right[rows, :][:, :cut])
        gap = jnp.zeros((BLK, cut), jnp.bfloat16)
        x_ref[rows, :] = joined(upper[rows, :][:, cut:], gap)
        gap = jnp.zeros((BLK, half - cut), jnp.bfloat16)
        y_ref[rows, :] = joined(gap, lower[rows, :][:, :cut])
    block = lax.broadcasted_iota(jnp.int32, (block_rows, half), 0)
    lane = lax.broadcasted_iota(jnp.int32, (block_rows, half), 1) // BLK

    def weight(ref):
        values = ref[pl.ds(height, block_rows), :].astype(jnp.float32)
        return jnp.sum(jnp.where(block == lane, values, 0.0), axis=0, keepdims=True)

    kept = jnp.sum(eye_sum(square, 0))
    own = weighted_diagonal(square, square, weight(left))
    across = weighted_diagonal(x_ref, y_ref, weight(upper))
    across += weighted_diagonal(y_ref, x_ref, weight(lower))
    lane = lax.broadcasted_iota(jnp.int32, out_ref.shape, 2)
    out_ref[...] = jnp.where(lane == 0, kept, jnp.where(lane == 1, own, across))


def partial_traces(scalars, own_a, own_b, near, copies):
    rows, half = own_a.shape
    anywhere = pl.BlockSpec(memory_space=pl.ANY)
    return pl.pallas_call(
        trace_kernel,
        out_shape=jax.ShapeDtypeStruct((copies, 1, LANES), jnp.float32),
        in_specs=[pl.BlockSpec(memory_space=pltpu.SMEM)] + [anywhere] * 3,
        out_specs=pl.BlockSpec(memory_space=pltpu.VMEM),
        scratch_shapes=[pltpu.VMEM((rows, half), jnp.bfloat16)] * 4
        + [pltpu.VMEM((half, half), jnp.bfloat16)] * 3
        + [pltpu.SemaphoreType.DMA((4,))],
        compiler_params=pltpu.CompilerParams(vmem_limit_bytes=24 * 1024 * 1024),
        cost_estimate=pl.CostEstimate(flops=10**9, bytes_accessed=2 * 10**6, transcendentals=0),
        name="partial_traces",
    )(scalars, own_a, own_b, near)


def total_kernel(scalars, sums, out_ref):
    values = sums[:, 0, :]
    moved = pltpu.roll(values, values.shape[0] - 1, 0)
    moved = jnp.where(scalars[0] == 0, moved, values)
    lane = lax.broadcasted_iota(jnp.int32, (1, LANES), 1)
    total = jnp.sum(values, axis=0, keepdims=True)
    across = jnp.sum(moved, axis=0, keepdims=True)
    order = (scalars[2] * BLK).astype(jnp.float32)

    def pick(row, k):
        return jnp.sum(jnp.where(lane == k, row, 0.0))

    out_ref[0] = pick(total, 0) / order
    out_ref[1] = (pick(total, 1) + pick(across, 2)) / order


def total(scalars, sums):
    return pl.pallas_call(
        total_kernel,
        out_shape=jax.ShapeDtypeStruct((2,), jnp.float32),
        in_specs=[
            pl.BlockSpec(memory_space=pltpu.SMEM),
            pl.BlockSpec(memory_space=pltpu.VMEM),
        ],
        out_specs=pl.BlockSpec(memory_space=pltpu.SMEM),
        compiler_params=pltpu.CompilerParams(vmem_limit_bytes=8 * 1024 * 1024),
        name="total",
    )(scalars, sums)


def purify_kernel(
    scalars, filter_ref, own_a, own_b, near, near_b, far, far_b,
    out_ref, band, full, sq, fmask, cube, sems,
):
    height, half = out_ref.shape
    block_rows = height // BLK
    slots = 2 * half // BLK
    col = scalars[0]
    mine = pl.multiple_of(col * half, half)
    other = pl.multiple_of((1 - col) * half, half)
    inner = 2 * col
    places = (
        (own_a, 1, mine), (own_b, 1, other), (near, inner, other),
        (near_b, 2 - inner, mine), (far, 2 - inner, other), (far_b, inner, mine),
    )
    copies = []
    for k, (src, row, lane) in enumerate(places):
        start = pl.multiple_of(row * height, height)
        copy = pltpu.make_async_copy(
            src.at[pl.ds(0, height), :],
            band.at[pl.ds(start, height), pl.ds(lane, half)],
            sems.at[k],
        )
        copy.start()
        copies.append(copy)
    width = full.shape[1]
    valid = own_valid(scalars, block_rows, 0, slots, slots // 2)
    wide = spread(jnp.where(valid, filter_ref[...], 0), slots * BLK)
    for i in range(block_rows):
        fmask[pl.ds(i, 1), :] = placed(wide[i : i + 1], i * BLK, width)

    def skew(row):
        for r in range(row * block_rows, (row + 1) * block_rows):
            rows = band[pl.ds(r * BLK, BLK), :]
            full[pl.ds(r * BLK, BLK), :] = placed(rows, (r - block_rows) * BLK, width)

    copies[0].wait()
    copies[1].wait()
    skew(1)
    for copy in copies[2:]:
        copy.wait()
    skew(0)
    skew(2)
    tiles = height // TILE
    span = (block_rows * 2 + TILE // BLK - 1) * BLK
    span = -(-span // TILE)
    reach = height // TILE
    per_tile = TILE // BLK
    sq[...] = jnp.zeros_like(sq)
    for m in range(tiles):
        for b in range(m, m + span):
            first = max(b - reach, m)
            last = min(b + reach, m + span - 1)
            k0, klen = first * TILE, (last - first + 1) * TILE
            prod = jnp.dot(
                full[pl.ds(height + m * TILE, TILE), pl.ds(k0, klen)],
                full[pl.ds(k0, klen), pl.ds(b * TILE, TILE)],
                preferred_element_type=jnp.float32,
            )
            for i in range(per_tile):
                row = m * per_tile + i
                keep = fmask[pl.ds(row, 1), pl.ds(b * TILE, TILE)]
                sq[pl.ds(row * BLK, BLK), pl.ds(b * TILE, TILE)] = (
                    prod[i * BLK : (i + 1) * BLK] * keep
                ).astype(jnp.bfloat16)
    out_span = half // TILE + 1
    for m in range(tiles):
        lanes = pl.multiple_of(m * TILE + col * half, TILE)
        cube[...] = jnp.dot(
            sq[pl.ds(m * TILE, TILE), pl.ds(m * TILE, span * TILE)],
            full[pl.ds(m * TILE, span * TILE), pl.ds(lanes, out_span * TILE)],
            preferred_element_type=jnp.float32,
        )
        for i in range(per_tile):
            row = m * per_tile + i
            base = i * BLK // LANES * LANES
            shift = i * BLK - base
            size = half + (LANES if shift else 0)
            at = pl.ds(pl.multiple_of(m * TILE + base + col * half, LANES), size)
            kept = sq[pl.ds(row * BLK, BLK), at].astype(jnp.float32)
            keep = fmask[pl.ds(row, 1), at]
            part = cube[pl.ds(i * BLK, BLK), pl.ds(base, size)]
            result = (3.0 * kept - 2.0 * (part * keep)).astype(jnp.bfloat16)
            out_ref[pl.ds(row * BLK, BLK), :] = result[:, shift : shift + half]


def purify(scalars, keep_filter, height, *pieces):
    half = pieces[0].shape[1]
    width = 3 * height
    block_rows = height // BLK
    anywhere = pl.BlockSpec(memory_space=pl.ANY)
    vmem = pl.BlockSpec(memory_space=pltpu.VMEM)
    return pl.pallas_call(
        purify_kernel,
        out_shape=jax.ShapeDtypeStruct((height, half), jnp.bfloat16),
        in_specs=[pl.BlockSpec(memory_space=pltpu.SMEM), vmem] + [anywhere] * 6,
        out_specs=vmem,
        scratch_shapes=[
            pltpu.VMEM((width, 2 * half), jnp.bfloat16),
            pltpu.VMEM((width, width), jnp.bfloat16),
            pltpu.VMEM((height, width), jnp.bfloat16),
            pltpu.VMEM((block_rows, width), jnp.float32),
            pltpu.VMEM((TILE, half + TILE), jnp.float32),
            pltpu.SemaphoreType.DMA((6,)),
        ],
        compiler_params=pltpu.CompilerParams(vmem_limit_bytes=48 * 1024 * 1024),
        cost_estimate=pl.CostEstimate(flops=3 * 10**9, bytes_accessed=4 * 10**6, transcendentals=0),
        name="purify",
    )(scalars, keep_filter, *pieces)


def per_device(density, pattern, filter_mask):
    block_rows = pattern.shape[0]
    size = lax.axis_size("row")
    row, col = lax.axis_index("row"), lax.axis_index("col")
    scalars = jnp.stack([col, row * block_rows, size * block_rows * jnp.ones_like(row)]).astype(jnp.int32)
    kept = keep(scalars, density, pattern, filter_mask)

    def device(row, col):
        return 2 * row + col

    def exchanged(value, upper_col):
        pairs = [
            (device(i, upper_col), device(i + 1, 1 - upper_col)) for i in range(size - 1)
        ]
        return lax.ppermute(value, ("row", "col"), pairs + [(b, a) for a, b in pairs])

    def swapped(value):
        return lax.ppermute(value, "col", [(0, 1), (1, 0)])

    near = exchanged(kept, 1)
    own_b = swapped(kept)
    far = exchanged(kept, 0)
    sums = partial_traces(scalars, kept, own_b, near, size)
    sums = lax.all_to_all(sums, "row", split_axis=0, concat_axis=0, tiled=True)
    near_b = swapped(near)
    far_b = swapped(far)
    purified = purify(scalars, filter_mask, density.shape[0], kept, own_b, near, near_b, far, far_b)
    return purified, total(scalars, sums)


def solution(mesh):
    placed_as = (P(SNAP_ROW, "col"), P(SNAP_ROW, "col"), P(SNAP_ROW, None))
    return jax.shard_map(
        per_device,
        mesh=mesh,
        in_specs=placed_as,
        out_specs=(P(SNAP_ROW, "col"), P("snap")),
        check_vma=False,
    )
```

```python
import functools

import jax
import jax.numpy as jnp
from jax import lax
from jax.experimental import pallas as pl
from jax.experimental.pallas import tpu as pltpu
from jax.sharding import PartitionSpec as P


BLK = 32
LANES = 128
TILE = 256
SNAP_ROW = ("snap", "row")


def spread(mask, width):
    slots = mask.shape[1]
    slot = lax.broadcasted_iota(jnp.int32, (slots, width), 0)
    lane = lax.broadcasted_iota(jnp.int32, (slots, width), 1)
    chosen = (lane // BLK == slot).astype(jnp.bfloat16)
    return jnp.dot(
        mask.astype(jnp.bfloat16), chosen, preferred_element_type=jnp.float32
    )


def placed(rows, start, width):
    height, length = rows.shape
    if start < 0:
        rows = rows[:, -start:]
        length += start
        start = 0
    if start + length > width:
        length = width - start
        rows = rows[:, :length]
    parts = []
    if start:
        parts.append(jnp.zeros((height, start), rows.dtype))
    parts.append(rows)
    if start + length < width:
        parts.append(jnp.zeros((height, width - start - length), rows.dtype))
    return jnp.concatenate(parts, 1) if len(parts) > 1 else rows


def eye_sum(ref, lane_start):
    row = lax.broadcasted_iota(jnp.int32, (LANES, LANES), 0)
    lane = lax.broadcasted_iota(jnp.int32, (LANES, LANES), 1)
    total = jnp.zeros((1, LANES), jnp.float32)
    for k in range(ref.shape[0] // LANES):
        part = ref[pl.ds(k * LANES, LANES), pl.ds(lane_start + k * LANES, LANES)]
        part = jnp.where(row == lane, part.astype(jnp.float32), 0.0)
        total += jnp.sum(part, axis=0, keepdims=True)
    return total


def own_valid(block_rows, first_slot, slots, half_band):
    row = lax.broadcasted_iota(jnp.int32, (block_rows, slots), 0)
    slot = lax.broadcasted_iota(jnp.int32, (block_rows, slots), 1)
    column = lax.axis_index("row") * block_rows + row + first_slot + slot - half_band
    return (column >= 0) & (column < lax.axis_size("row") * block_rows)


def slot_kernel(chosen):
    slot = lax.broadcasted_iota(jnp.int32, chosen.shape, 0)
    lane = lax.broadcasted_iota(jnp.int32, chosen.shape, 1)
    chosen[...] = (lane // BLK == slot).astype(jnp.bfloat16)


def mask_kernel(chosen, pattern, keep_filter, mask):
    block_rows, slots = pattern.shape
    half = mask.shape[1]
    valid = own_valid(block_rows, lax.axis_index("col") * slots, slots, slots)
    own = jnp.where(valid, pattern[...], 0).astype(jnp.bfloat16)
    wide = jnp.dot(own, chosen[...], preferred_element_type=jnp.float32)
    mask[pl.ds(0, block_rows), :] = wide.astype(jnp.bfloat16)
    slot = lax.broadcasted_iota(jnp.int32, keep_filter.shape, 1)
    on_diagonal = jnp.where(slot == slots, keep_filter[...], 0).astype(jnp.float32)
    on_diagonal = jnp.sum(on_diagonal, axis=1, keepdims=True)
    mask[pl.ds(block_rows, block_rows), :] = jnp.broadcast_to(
        on_diagonal, (block_rows, half)
    ).astype(jnp.bfloat16)


def keep_kernel(density, mask, kept):
    height = density.shape[0]
    block_rows = height // BLK
    for i in range(block_rows):
        rows = pl.ds(i * BLK, BLK)
        kept[rows, :] = density[rows, :] * mask[pl.ds(i, 1), :]
    kept[pl.ds(height, block_rows), :] = mask[pl.ds(block_rows, block_rows), :]


def small_call(kernel, shape, scratch, flops, *operands, dtype=jnp.float32):
    vmem = pl.BlockSpec(memory_space=pltpu.VMEM)
    return pl.pallas_call(
        kernel,
        out_shape=jax.ShapeDtypeStruct(shape, dtype),
        in_specs=[vmem] * len(operands),
        out_specs=vmem,
        scratch_shapes=scratch,
        compiler_params=pltpu.CompilerParams(vmem_limit_bytes=16 * 1024 * 1024),
        cost_estimate=pl.CostEstimate(flops=flops, bytes_accessed=10**6, transcendentals=0),
    )(*operands)


def keep(density, pattern, keep_filter):
    height, half = density.shape
    block_rows = pattern.shape[0]
    chosen = small_call(slot_kernel, (pattern.shape[1], half), (), 10**10, dtype=density.dtype)
    mask = small_call(
        mask_kernel, (2 * block_rows, half), (), 10**3, chosen, pattern, keep_filter,
        dtype=density.dtype,
    )
    return small_call(
        keep_kernel, (height + block_rows, half), (), 10**9, density, mask,
        dtype=density.dtype,
    )


def joined(left, right):
    parts = [part for part in (left, right) if part.shape[1]]
    return jnp.concatenate(parts, 1) if len(parts) > 1 else parts[0]


def weighted_diagonal(a, b, weight):
    total = jnp.zeros((1, TILE), jnp.float32)
    row = lax.broadcasted_iota(jnp.int32, (TILE, TILE), 0)
    lane = lax.broadcasted_iota(jnp.int32, (TILE, TILE), 1)
    for m in range(a.shape[0] // TILE):
        at = pl.ds(m * TILE, TILE)
        prod = jnp.dot(a[at, :], b[:, at], preferred_element_type=jnp.float32)
        diagonal = jnp.sum(jnp.where(row == lane, prod, 0.0), axis=0, keepdims=True)
        total += diagonal * weight[:, m * TILE : (m + 1) * TILE]
    return jnp.sum(total)


def diagonal_weight(values):
    block = lax.broadcasted_iota(jnp.int32, values.shape, 0)
    lane = lax.broadcasted_iota(jnp.int32, values.shape, 1) // BLK
    values = jnp.where(block == lane, values.astype(jnp.float32), 0.0)
    return jnp.sum(values, axis=0, keepdims=True)


def inner_kernel(own_a, own_b, out_ref, square):
    half = own_a.shape[1]
    height = square.shape[0]
    block_rows = height // BLK
    first = lax.axis_index("col") == 0
    for i in range(block_rows):
        rows = pl.ds(i * BLK, BLK)
        cut = half - i * BLK
        a, b = own_a[rows, :], own_b[rows, :]
        left, right = jnp.where(first, a, b), jnp.where(first, b, a)
        square[rows, :] = joined(left[:, cut:], right[:, :cut])
    weight = diagonal_weight(own_a[pl.ds(height, block_rows), :])
    kept = jnp.sum(eye_sum(square, 0))
    inner = weighted_diagonal(square, square, weight)
    lane = lax.broadcasted_iota(jnp.int32, out_ref.shape, 1)
    out_ref[...] = jnp.where(lane == 0, kept, jnp.where(lane == 1, inner, 0.0))


def across_kernel(own_a, near, inner, out_ref, x_ref, y_ref):
    half = own_a.shape[1]
    height = x_ref.shape[0]
    block_rows = height // BLK
    first = lax.axis_index("col") == 0
    for i in range(block_rows):
        rows = pl.ds(i * BLK, BLK)
        cut = half - i * BLK
        a, b = own_a[rows, :], near[rows, :]
        upper, lower = jnp.where(first, b, a), jnp.where(first, a, b)
        gap = jnp.zeros((BLK, cut), jnp.bfloat16)
        x_ref[rows, :] = joined(upper[:, cut:], gap)
        gap = jnp.zeros((BLK, half - cut), jnp.bfloat16)
        y_ref[rows, :] = joined(gap, lower[:, :cut])
    below = pl.ds(height, block_rows)
    a, b = own_a[below, :], near[below, :]
    across = weighted_diagonal(x_ref, y_ref, diagonal_weight(jnp.where(first, b, a)))
    across += weighted_diagonal(y_ref, x_ref, diagonal_weight(jnp.where(first, a, b)))
    lane = lax.broadcasted_iota(jnp.int32, out_ref.shape, 1)
    out_ref[...] = jnp.where(lane == 2, across, inner[0:1, :])


def total_kernel(order, sums, out_ref):
    values = sums[...]
    moved = pltpu.roll(values, values.shape[0] - 1, 0)
    lane = lax.broadcasted_iota(jnp.int32, values.shape, 1)
    moves = lane + 128 * lax.axis_index("col") == 2
    values = jnp.sum(jnp.where(moves, moved, values), axis=0, keepdims=True)
    after = pltpu.roll(values, LANES - 1, 1)
    lane = lax.broadcasted_iota(jnp.int32, values.shape, 1)
    out_ref[...] = (jnp.where(lane == 1, values + after, values) / order)[0, :2]


def total(sums, order):
    vmem = pl.BlockSpec(memory_space=pltpu.VMEM)
    return pl.pallas_call(
        functools.partial(total_kernel, order),
        out_shape=jax.ShapeDtypeStruct((2,), jnp.float32),
        in_specs=[vmem],
        out_specs=vmem,
        compiler_params=pltpu.CompilerParams(vmem_limit_bytes=8 * 1024 * 1024),
        name="total",
    )(sums)


def purify_kernel(
    filter_ref, own_a, own_b, near, near_b, far, far_b,
    out_ref, band, full, sq, fmask, cube, sems,
):
    height, half = out_ref.shape
    block_rows = height // BLK
    slots = 2 * half // BLK
    col = lax.axis_index("col")
    mine = pl.multiple_of(col * half, half)
    other = pl.multiple_of((1 - col) * half, half)
    inner = 2 * col
    places = (
        (own_a, 1, mine), (own_b, 1, other), (near, inner, other),
        (near_b, 2 - inner, mine), (far, inner, mine), (far_b, 2 - inner, other),
    )
    copies = []
    for k, (src, row, lane) in enumerate(places):
        start = pl.multiple_of(row * height, height)
        copy = pltpu.make_async_copy(
            src.at[pl.ds(0, height), :],
            band.at[pl.ds(start, height), pl.ds(lane, half)],
            sems.at[k],
        )
        copy.start()
        copies.append(copy)
    width = full.shape[1]
    valid = own_valid(block_rows, 0, slots, slots // 2)
    wide = spread(jnp.where(valid, filter_ref[...], 0), slots * BLK)
    for i in range(block_rows):
        fmask[pl.ds(i, 1), :] = placed(wide[i : i + 1], i * BLK, width)

    def skew(row):
        for r in range(row * block_rows, (row + 1) * block_rows):
            rows = band[pl.ds(r * BLK, BLK), :]
            full[pl.ds(r * BLK, BLK), :] = placed(rows, (r - block_rows) * BLK, width)

    copies[0].wait()
    copies[1].wait()
    skew(1)
    for copy in copies[2:]:
        copy.wait()
    skew(0)
    skew(2)
    tiles = height // TILE
    span = (block_rows * 2 + TILE // BLK - 1) * BLK
    span = -(-span // TILE)
    reach = height // TILE
    per_tile = TILE // BLK
    sq[...] = jnp.zeros_like(sq)
    for m in range(tiles):
        for b in range(m, m + span):
            first = max(b - reach, m)
            last = min(b + reach, m + span - 1)
            k0, klen = first * TILE, (last - first + 1) * TILE
            prod = jnp.dot(
                full[pl.ds(height + m * TILE, TILE), pl.ds(k0, klen)],
                full[pl.ds(k0, klen), pl.ds(b * TILE, TILE)],
                preferred_element_type=jnp.float32,
            )
            for i in range(per_tile):
                row = m * per_tile + i
                keep = fmask[pl.ds(row, 1), pl.ds(b * TILE, TILE)]
                sq[pl.ds(row * BLK, BLK), pl.ds(b * TILE, TILE)] = (
                    prod[i * BLK : (i + 1) * BLK] * keep
                ).astype(jnp.bfloat16)
    out_span = half // TILE + 1
    for m in range(tiles):
        lanes = pl.multiple_of(m * TILE + col * half, TILE)
        cube[...] = jnp.dot(
            sq[pl.ds(m * TILE, TILE), pl.ds(m * TILE, span * TILE)],
            full[pl.ds(m * TILE, span * TILE), pl.ds(lanes, out_span * TILE)],
            preferred_element_type=jnp.float32,
        )
        for i in range(per_tile):
            row = m * per_tile + i
            base = i * BLK // LANES * LANES
            shift = i * BLK - base
            size = half + (LANES if shift else 0)
            at = pl.ds(pl.multiple_of(m * TILE + base + col * half, LANES), size)
            kept = sq[pl.ds(row * BLK, BLK), at].astype(jnp.float32)
            keep = fmask[pl.ds(row, 1), at]
            part = cube[pl.ds(i * BLK, BLK), pl.ds(base, size)]
            result = (3.0 * kept - 2.0 * (part * keep)).astype(jnp.bfloat16)
            out_ref[pl.ds(row * BLK, BLK), :] = result[:, shift : shift + half]


def purify(keep_filter, height, *pieces):
    half = pieces[0].shape[1]
    width = 3 * height
    block_rows = height // BLK
    anywhere = pl.BlockSpec(memory_space=pl.ANY)
    vmem = pl.BlockSpec(memory_space=pltpu.VMEM)
    return pl.pallas_call(
        purify_kernel,
        out_shape=jax.ShapeDtypeStruct((height, half), jnp.bfloat16),
        in_specs=[vmem] + [anywhere] * 6,
        out_specs=vmem,
        scratch_shapes=[
            pltpu.VMEM((width, 2 * half), jnp.bfloat16),
            pltpu.VMEM((width, width), jnp.bfloat16),
            pltpu.VMEM((height, width), jnp.bfloat16),
            pltpu.VMEM((block_rows, width), jnp.float32),
            pltpu.VMEM((TILE, half + TILE), jnp.float32),
            pltpu.SemaphoreType.DMA((6,)),
        ],
        compiler_params=pltpu.CompilerParams(vmem_limit_bytes=48 * 1024 * 1024),
        cost_estimate=pl.CostEstimate(flops=3 * 10**9, bytes_accessed=4 * 10**6, transcendentals=0),
        name="purify",
    )(keep_filter, *pieces)


def per_device(density, pattern, filter_mask):
    size = lax.axis_size("row")
    kept = keep(density, pattern, filter_mask)

    def device(row, col):
        return 2 * row + col

    def exchanged(value):
        pairs = [(device(i, 1), device(i + 1, 0)) for i in range(size - 1)]
        return lax.ppermute(value, ("row", "col"), pairs + [(b, a) for a, b in pairs])

    def shifted(value):
        pairs = [(device(i, 0), device(i + 1, 0)) for i in range(size - 1)]
        pairs += [(device(i + 1, 1), device(i, 1)) for i in range(size - 1)]
        return lax.ppermute(value, ("row", "col"), pairs)

    def swapped(value):
        return lax.ppermute(value, "col", [(0, 1), (1, 0)])

    half = density.shape[1]
    square = pltpu.VMEM((half, half), jnp.bfloat16)
    near = exchanged(kept)
    own_b = swapped(kept)
    sums = small_call(inner_kernel, (8, LANES), [square], 10**9, kept, own_b)
    far = shifted(kept)
    sums = small_call(across_kernel, (size, LANES), [square] * 2, 10**9, kept, near, sums)
    sums = sums.reshape(size, 1, LANES)
    sums = lax.all_to_all(sums, "row", split_axis=0, concat_axis=0, tiled=True)
    sums = sums.reshape(size, LANES)
    near_b = swapped(near)
    far_b = swapped(far)
    purified = purify(
        filter_mask, density.shape[0], kept, own_b, near, near_b, far, far_b
    )
    return purified, total(sums, size * density.shape[0])


def solution(mesh):
    placed_as = (P(SNAP_ROW, "col"), P(SNAP_ROW, "col"), P(SNAP_ROW, None))
    return jax.shard_map(
        per_device,
        mesh=mesh,
        in_specs=placed_as,
        out_specs=(P(SNAP_ROW, "col"), P("snap")),
        check_vma=False,
    )
```

```python
import functools

import jax
import jax.numpy as jnp
from jax import lax
from jax.experimental import pallas as pl
from jax.experimental.pallas import tpu as pltpu
from jax.sharding import PartitionSpec as P


BLK = 32
LANES = 128
TILE = 256
SNAP_ROW = ("snap", "row")


def spread(mask, width):
    slots = mask.shape[1]
    slot = lax.broadcasted_iota(jnp.int32, (slots, width), 0)
    lane = lax.broadcasted_iota(jnp.int32, (slots, width), 1)
    chosen = (lane // BLK == slot).astype(jnp.bfloat16)
    return jnp.dot(
        mask.astype(jnp.bfloat16), chosen, preferred_element_type=jnp.float32
    )


def placed(rows, start, width):
    height, length = rows.shape
    if start < 0:
        rows = rows[:, -start:]
        length += start
        start = 0
    if start + length > width:
        length = width - start
        rows = rows[:, :length]
    parts = []
    if start:
        parts.append(jnp.zeros((height, start), rows.dtype))
    parts.append(rows)
    if start + length < width:
        parts.append(jnp.zeros((height, width - start - length), rows.dtype))
    return jnp.concatenate(parts, 1) if len(parts) > 1 else rows


def eye_sum(ref, lane_start):
    row = lax.broadcasted_iota(jnp.int32, (LANES, LANES), 0)
    lane = lax.broadcasted_iota(jnp.int32, (LANES, LANES), 1)
    total = jnp.zeros((1, LANES), jnp.float32)
    for k in range(ref.shape[0] // LANES):
        part = ref[pl.ds(k * LANES, LANES), pl.ds(lane_start + k * LANES, LANES)]
        part = jnp.where(row == lane, part.astype(jnp.float32), 0.0)
        total += jnp.sum(part, axis=0, keepdims=True)
    return total


def own_valid(block_rows, first_slot, slots, half_band):
    row = lax.broadcasted_iota(jnp.int32, (block_rows, slots), 0)
    slot = lax.broadcasted_iota(jnp.int32, (block_rows, slots), 1)
    column = lax.axis_index("row") * block_rows + row + first_slot + slot - half_band
    return (column >= 0) & (column < lax.axis_size("row") * block_rows)


def slot_kernel(chosen):
    slot = lax.broadcasted_iota(jnp.int32, chosen.shape, 0)
    lane = lax.broadcasted_iota(jnp.int32, chosen.shape, 1)
    chosen[...] = (lane // BLK == slot).astype(jnp.bfloat16)


def mask_kernel(chosen, pattern, keep_filter, mask):
    block_rows, slots = pattern.shape
    half = mask.shape[1]
    valid = own_valid(block_rows, lax.axis_index("col") * slots, slots, slots)
    own = jnp.where(valid, pattern[...], 0).astype(jnp.bfloat16)
    wide = jnp.dot(own, chosen[...], preferred_element_type=jnp.float32)
    mask[pl.ds(0, block_rows), :] = wide.astype(jnp.bfloat16)
    slot = lax.broadcasted_iota(jnp.int32, keep_filter.shape, 1)
    on_diagonal = jnp.where(slot == slots, keep_filter[...], 0).astype(jnp.float32)
    on_diagonal = jnp.sum(on_diagonal, axis=1, keepdims=True)
    mask[pl.ds(block_rows, block_rows), :] = jnp.broadcast_to(
        on_diagonal, (block_rows, half)
    ).astype(jnp.bfloat16)


def keep_kernel(density, mask, kept):
    height = density.shape[0]
    block_rows = height // BLK
    for i in range(block_rows):
        rows = pl.ds(i * BLK, BLK)
        kept[rows, :] = density[rows, :] * mask[pl.ds(i, 1), :]
    kept[pl.ds(height, block_rows), :] = mask[pl.ds(block_rows, block_rows), :]


def small_call(kernel, shape, scratch, flops, *operands, dtype=jnp.float32):
    vmem = pl.BlockSpec(memory_space=pltpu.VMEM)
    return pl.pallas_call(
        kernel,
        out_shape=jax.ShapeDtypeStruct(shape, dtype),
        in_specs=[vmem] * len(operands),
        out_specs=vmem,
        scratch_shapes=scratch,
        compiler_params=pltpu.CompilerParams(vmem_limit_bytes=16 * 1024 * 1024),
        cost_estimate=pl.CostEstimate(flops=flops, bytes_accessed=10**6, transcendentals=0),
    )(*operands)


def keep(density, pattern, keep_filter):
    height, half = density.shape
    block_rows = pattern.shape[0]
    chosen = small_call(slot_kernel, (pattern.shape[1], half), (), 10**10, dtype=density.dtype)
    mask = small_call(
        mask_kernel, (2 * block_rows, half), (), 10**3, chosen, pattern, keep_filter,
        dtype=density.dtype,
    )
    return small_call(
        keep_kernel, (height + block_rows, half), (), 10**9, density, mask,
        dtype=density.dtype,
    )


def joined(left, right):
    parts = [part for part in (left, right) if part.shape[1]]
    return jnp.concatenate(parts, 1) if len(parts) > 1 else parts[0]


def weighted_diagonal(a, b, weight):
    total = jnp.zeros((1, TILE), jnp.float32)
    row = lax.broadcasted_iota(jnp.int32, (TILE, TILE), 0)
    lane = lax.broadcasted_iota(jnp.int32, (TILE, TILE), 1)
    for m in range(a.shape[0] // TILE):
        at = pl.ds(m * TILE, TILE)
        prod = jnp.dot(a[at, :], b[:, at], preferred_element_type=jnp.float32)
        diagonal = jnp.sum(jnp.where(row == lane, prod, 0.0), axis=0, keepdims=True)
        total += diagonal * weight[:, m * TILE : (m + 1) * TILE]
    return jnp.sum(total)


def diagonal_weight(values):
    block = lax.broadcasted_iota(jnp.int32, values.shape, 0)
    lane = lax.broadcasted_iota(jnp.int32, values.shape, 1) // BLK
    values = jnp.where(block == lane, values.astype(jnp.float32), 0.0)
    return jnp.sum(values, axis=0, keepdims=True)


def pack_kernel(own_a, packed):
    half = own_a.shape[1]
    block_rows = half // BLK

    def pair(k):
        at = block_rows - 1 - k
        return own_a[pl.ds(k * BLK, BLK), :], own_a[pl.ds(at * BLK, BLK), :]

    @pl.when(lax.axis_index("col") == 0)
    def _():
        for k in range(block_rows // 2):
            a, b = pair(k)
            packed[pl.ds(k * BLK, BLK), :] = joined(a[:, half - k * BLK :], b[:, k * BLK :])

    @pl.when(lax.axis_index("col") != 0)
    def _():
        for k in range(block_rows // 2):
            a, b = pair(k)
            packed[pl.ds(k * BLK, BLK), :] = joined(a[:, : half - k * BLK], b[:, : k * BLK])


def split_kernel(own_a, early, late):
    half = own_a.shape[1]
    block_rows = half // BLK
    early[pl.ds(half // 2, block_rows), :] = own_a[pl.ds(half, block_rows), :]

    def pair(k):
        at = block_rows - 1 - k
        return own_a[pl.ds(k * BLK, BLK), :], own_a[pl.ds(at * BLK, BLK), :]

    @pl.when(lax.axis_index("col") != 0)
    def _():
        for k in range(block_rows // 2):
            (a, b), rows, cut = pair(k), pl.ds(k * BLK, BLK), k * BLK
            early[rows, :] = joined(a[:, half - cut :], b[:, cut:])
            late[rows, :] = joined(a[:, : half - cut], b[:, :cut])

    @pl.when(lax.axis_index("col") == 0)
    def _():
        for k in range(block_rows // 2):
            (a, b), rows, cut = pair(k), pl.ds(k * BLK, BLK), k * BLK
            early[rows, :] = joined(a[:, BLK : half - cut], b[:, : cut + BLK])
            late[rows, :] = joined(joined(a[:, :BLK], a[:, half - cut :]), b[:, cut + BLK :])


def split(own_a):
    rows, half = own_a.shape
    vmem = pl.BlockSpec(memory_space=pltpu.VMEM)
    return pl.pallas_call(
        split_kernel,
        out_shape=(
            jax.ShapeDtypeStruct((rows - half // 2, half), own_a.dtype),
            jax.ShapeDtypeStruct((half // 2, half), own_a.dtype),
        ),
        in_specs=[vmem],
        out_specs=(vmem, vmem),
        compiler_params=pltpu.CompilerParams(vmem_limit_bytes=16 * 1024 * 1024),
        cost_estimate=pl.CostEstimate(flops=10**8, bytes_accessed=10**6, transcendentals=0),
        name="split",
    )(own_a)


def stack_kernel(early, late, both):
    rows = late.shape[0]
    both[pl.ds(0, rows), :] = late[...]
    both[pl.ds(rows, early.shape[0]), :] = early[...]


def inner_kernel(own_a, own_b, out_ref, square):
    half = own_a.shape[1]
    height = square.shape[0]
    block_rows = height // BLK
    first = lax.axis_index("col") == 0
    for i in range(block_rows):
        rows = pl.ds(i * BLK, BLK)
        cut = half - i * BLK
        a, b = own_a[rows, :], own_b[rows, :]
        left, right = jnp.where(first, a, b), jnp.where(first, b, a)
        square[rows, :] = joined(left[:, cut:], right[:, :cut])
    weight = diagonal_weight(own_a[pl.ds(height, block_rows), :])
    kept = jnp.sum(eye_sum(square, 0))
    inner = weighted_diagonal(square, square, weight)
    lane = lax.broadcasted_iota(jnp.int32, out_ref.shape, 1)
    out_ref[...] = jnp.where(lane == 0, kept, jnp.where(lane == 1, inner, 0.0))


def across_kernel(own_a, near, inner, out_ref, x_ref, y_ref):
    half = own_a.shape[1]
    block_rows = half // BLK

    def rows(i):
        return pl.ds(i * BLK, BLK)

    def gap(blocks):
        return jnp.zeros((BLK, blocks * BLK), jnp.bfloat16)

    @pl.when(lax.axis_index("col") == 0)
    def _():
        for k in range(block_rows // 2):
            i, cut, piece = block_rows - 1 - k, k * BLK, near[rows(k), :]
            x_ref[rows(k), :] = joined(piece[:, :cut], gap(block_rows - k))
            x_ref[rows(i), :] = joined(piece[:, cut + BLK :], gap(k + 1))
        for i in range(block_rows):
            y_ref[rows(i), :] = joined(gap(i), own_a[rows(i), :][:, : half - i * BLK])

    @pl.when(lax.axis_index("col") != 0)
    def _():
        for i in range(block_rows):
            x_ref[rows(i), :] = joined(own_a[rows(i), :][:, half - i * BLK :], gap(block_rows - i))
        for k in range(block_rows // 2):
            i, piece = block_rows - 1 - k, near[rows(k), :]
            y_ref[rows(k), :] = joined(gap(k + 1), piece[:, : i * BLK])
            y_ref[rows(i), :] = joined(gap(i), piece[:, i * BLK :])

    first = lax.axis_index("col") == 0
    a = own_a[pl.ds(half, block_rows), :]
    b = near[pl.ds(half // 2, block_rows), :]
    across = weighted_diagonal(x_ref, y_ref, diagonal_weight(jnp.where(first, b, a)))
    across += weighted_diagonal(y_ref, x_ref, diagonal_weight(jnp.where(first, a, b)))
    lane = lax.broadcasted_iota(jnp.int32, out_ref.shape, 1)
    out_ref[...] = jnp.where(lane == 2, across, inner[0:1, :])


def total_kernel(order, sums, out_ref):
    values = sums[...]
    moved = pltpu.roll(values, values.shape[0] - 1, 0)
    lane = lax.broadcasted_iota(jnp.int32, values.shape, 1)
    moves = lane + 128 * lax.axis_index("col") == 2
    values = jnp.sum(jnp.where(moves, moved, values), axis=0, keepdims=True)
    after = pltpu.roll(values, LANES - 1, 1)
    lane = lax.broadcasted_iota(jnp.int32, values.shape, 1)
    out_ref[...] = (jnp.where(lane == 1, values + after, values) / order)[0, :2]


def total(sums, order):
    vmem = pl.BlockSpec(memory_space=pltpu.VMEM)
    return pl.pallas_call(
        functools.partial(total_kernel, order),
        out_shape=jax.ShapeDtypeStruct((2,), jnp.float32),
        in_specs=[vmem],
        out_specs=vmem,
        compiler_params=pltpu.CompilerParams(vmem_limit_bytes=8 * 1024 * 1024),
        name="total",
    )(sums)


def purify_kernel(
    filter_ref, own_a, own_b, nearer, nearer_b, far, far_b,
    out_ref, full, sq, fmask, cube,
):
    height, half = out_ref.shape
    block_rows = height // BLK
    slots = 2 * half // BLK
    col = lax.axis_index("col")
    first = col == 0
    width = full.shape[1]
    valid = own_valid(block_rows, 0, slots, slots // 2)
    wide = spread(jnp.where(valid, filter_ref[...], 0), slots * BLK)
    for i in range(block_rows):
        fmask[pl.ds(i, 1), :] = placed(wide[i : i + 1], i * BLK, width)

    def lay(at, parts):
        gap = width - sum(part.shape[1] for part in parts)
        if gap:
            parts = parts + [jnp.zeros((BLK, gap), jnp.bfloat16)]
        parts = [part for part in parts if part.shape[1]]
        full[pl.ds(at * BLK, BLK), :] = jnp.concatenate(parts, 1)

    def gap(blocks):
        return jnp.zeros((BLK, blocks * BLK), jnp.bfloat16)

    def chosen(at_0, at_1, i):
        rows = pl.ds(i * BLK, BLK)
        return jnp.where(first, at_0[rows, :], at_1[rows, :])

    for i in range(block_rows):
        lay(block_rows + i, [gap(i), chosen(own_a, own_b, i), chosen(own_b, own_a, i)])
    below_k = block_rows // 2
    for k in range(block_rows // 2):
        i = block_rows - 1 - k
        cut = k * BLK
        before = chosen(far, far_b, k)
        late, early = chosen(nearer, nearer_b, k), chosen(nearer, nearer_b, below_k + k)
        lay(k, [before[:, :cut], late[:, : half - cut], early[:, :cut]])
        lay(i, [before[:, cut + BLK :], late[:, half - cut :], early[:, cut:]])
        after = chosen(far_b, far, k)
        late, early = chosen(nearer_b, nearer, k), chosen(nearer_b, nearer, below_k + k)
        below, split_at = 2 * block_rows, half - cut - BLK
        left = [late[:, :BLK], early[:, :split_at], late[:, BLK : cut + BLK]]
        lay(below + k, [gap(block_rows + k)] + left + [after[:, : half - cut]])
        left = [early[:, split_at:], late[:, cut + BLK :]]
        lay(below + i, [gap(block_rows + i)] + left + [after[:, half - cut :]])
    tiles = height // TILE
    span = (block_rows * 2 + TILE // BLK - 1) * BLK
    span = -(-span // TILE)
    reach = height // TILE
    per_tile = TILE // BLK
    for m in range(tiles):
        for b in range(m, m + span):
            first = max(b - reach, m)
            last = min(b + reach, m + span - 1)
            k0, klen = first * TILE, (last - first + 1) * TILE
            prod = jnp.dot(
                full[pl.ds(height + m * TILE, TILE), pl.ds(k0, klen)],
                full[pl.ds(k0, klen), pl.ds(b * TILE, TILE)],
                preferred_element_type=jnp.float32,
            )
            for i in range(per_tile):
                row = m * per_tile + i
                keep = fmask[pl.ds(row, 1), pl.ds(b * TILE, TILE)]
                sq[pl.ds(row * BLK, BLK), pl.ds(b * TILE, TILE)] = (
                    prod[i * BLK : (i + 1) * BLK] * keep
                ).astype(jnp.bfloat16)
    out_span = half // TILE + 1
    for m in range(tiles):
        lanes = pl.multiple_of(m * TILE + col * half, TILE)
        cube[...] = jnp.dot(
            sq[pl.ds(m * TILE, TILE), pl.ds(m * TILE, span * TILE)],
            full[pl.ds(m * TILE, span * TILE), pl.ds(lanes, out_span * TILE)],
            preferred_element_type=jnp.float32,
        )
        for i in range(per_tile):
            row = m * per_tile + i
            base = i * BLK // LANES * LANES
            shift = i * BLK - base
            size = half + (LANES if shift else 0)
            at = pl.ds(pl.multiple_of(m * TILE + base + col * half, LANES), size)
            kept = sq[pl.ds(row * BLK, BLK), at].astype(jnp.float32)
            keep = fmask[pl.ds(row, 1), at]
            part = cube[pl.ds(i * BLK, BLK), pl.ds(base, size)]
            result = (3.0 * kept - 2.0 * (part * keep)).astype(jnp.bfloat16)
            out_ref[pl.ds(row * BLK, BLK), :] = result[:, shift : shift + half]


def purify(keep_filter, height, *pieces):
    half = pieces[0].shape[1]
    width = 3 * height
    block_rows = height // BLK
    vmem = pl.BlockSpec(memory_space=pltpu.VMEM)
    return pl.pallas_call(
        purify_kernel,
        out_shape=jax.ShapeDtypeStruct((height, half), jnp.bfloat16),
        in_specs=[vmem] * 7,
        out_specs=vmem,
        scratch_shapes=[
            pltpu.VMEM((width, width), jnp.bfloat16),
            pltpu.VMEM((height, width), jnp.bfloat16),
            pltpu.VMEM((block_rows, width), jnp.float32),
            pltpu.VMEM((TILE, half + TILE), jnp.float32),
        ],
        compiler_params=pltpu.CompilerParams(vmem_limit_bytes=32 * 1024 * 1024,
        ),
        cost_estimate=pl.CostEstimate(flops=3 * 10**9, bytes_accessed=4 * 10**6, transcendentals=0),
        name="purify",
    )(keep_filter, *pieces)


def per_device(density, pattern, filter_mask):
    block_rows = pattern.shape[0]
    size = lax.axis_size("row")
    kept = keep(density, pattern, filter_mask)

    def device(row, col):
        return 2 * row + col

    def exchanged(value):
        pairs = [(device(i, 1), device(i + 1, 0)) for i in range(size - 1)]
        return lax.ppermute(value, ("row", "col"), pairs + [(b, a) for a, b in pairs])

    def shifted(value):
        pairs = [(device(i, 0), device(i + 1, 0)) for i in range(size - 1)]
        pairs += [(device(i + 1, 1), device(i, 1)) for i in range(size - 1)]
        return lax.ppermute(value, ("row", "col"), pairs)

    def swapped(value):
        return lax.ppermute(value, "col", [(0, 1), (1, 0)])

    half = density.shape[1]
    square = pltpu.VMEM((half, half), jnp.bfloat16)
    early, late = split(kept)
    near = exchanged(early)
    rest = exchanged(late)
    own_b = swapped(kept)
    packed = small_call(pack_kernel, (half // 2, half), (), 10**9, kept, dtype=kept.dtype)
    sums = small_call(inner_kernel, (8, LANES), [square], 10**9, kept, own_b)
    sums = small_call(across_kernel, (size, LANES), [square] * 2, 10**9, kept, near, sums)
    sums = sums.reshape(size, 1, LANES)
    sums = lax.all_to_all(sums, "row", split_axis=0, concat_axis=0, tiled=True)
    sums = sums.reshape(size, LANES)
    far = shifted(packed)
    nearer = small_call(
        stack_kernel, (half + block_rows, half), (), 10**8, near, rest,
        dtype=near.dtype,
    )
    nearer_b = swapped(nearer)
    far_b = swapped(far)
    purified = purify(
        filter_mask, density.shape[0], kept, own_b,
        nearer, nearer_b, far, far_b,
    )
    return purified, total(sums, size * density.shape[0])


def solution(mesh):
    placed_as = (P(SNAP_ROW, "col"), P(SNAP_ROW, "col"), P(SNAP_ROW, None))
    return jax.shard_map(
        per_device,
        mesh=mesh,
        in_specs=placed_as,
        out_specs=(P(SNAP_ROW, "col"), P("snap")),
        check_vma=False,
    )
```
